32 devices in a mesh: blocks: 2 (over y), gz: 8 (over z, x), gy: 2 (over core).
Axes of the slice: x: 2, y: 2, z: 4, core: 2. Of those that a mesh axis runs over, the one named last changes fastest.
Arguments:
- view_a: float32 [256, 32, 512], P(('blocks', 'gz'), 'gy'), parts along dimension 0, may hold values from 0.5 to 2
- view_b_own: float32 [1024, 32, 128], P(('blocks', 'gz'), 'gy'), parts along dimension 0, may hold values from 0.5 to 2
- spread_a: float32 [3, 31], replicated, may hold values from 0.05 to 1
- spread_b: float32 [3, 31], replicated, may hold values from 0.05 to 1
Outputs:
- estimate: float32 [256, 32, 512], P(('blocks', 'gz'), 'gy'), parts along dimension 0
The draws below stay inside these ranges and needn't reach their ends.
There are 2 independent parts, one for each index of `blocks`. The reference program is written for one: setup_inputs(seed, part) draws one part's arguments, and reference() takes and returns one part's arrays. A program takes and returns all parts, laid end to end along the dimension named above; an argument that names none is the same for every part. Nothing has to cross between parts.
All inputs are finite; a program needn't handle non-finite values.
Results may differ from the reference program's by a relative error of at most 0.0001.
Values sent between devices are 32-bit elements; how exact they have to be, the bound alone decides.
A program may use at most 64 MiB of HBM per device.

```python
import math
import jax
import jax.numpy as jnp
from jax import lax

NX = 512
R = 15
ITERS = 1
NZ = 128
NY = 32


def level_of(key, extent, split, smallest, high):
    gain, own = 1.0, jax.random.fold_in(key, 6)
    for position, blocks in split:
        steps = jnp.exp(jax.random.uniform(jax.random.fold_in(own, position), (blocks,), jnp.float32, smallest / len(split), high / len(split)))
        gain = gain * jnp.repeat(steps, extent[position] // blocks).reshape([-1 if axis == position else 1 for axis in range(len(extent))])
    return gain


def setup_inputs(seed: int = 0, part: int = 0) -> dict:
    key_of = jax.random.split(jax.random.key(seed), 5)
    own_keys = jax.random.split(jax.random.fold_in(key_of[4], part), 5)
    return {
        "view_a": jnp.clip(0.5 + 1.5 * jax.random.uniform(own_keys[0], (NZ, NY, NX), jnp.float32) ** level_of(own_keys[0], (NZ, NY, NX), ((0, 8), (1, 2)), -0.2, 0.2), 0.5, 2.0),
        "view_b_own": jnp.clip(0.5 + 1.5 * jax.random.uniform(own_keys[1], (NX, NY, NZ), jnp.float32) ** level_of(own_keys[1], (NX, NY, NZ), ((0, 8), (1, 2)), -0.2, 0.2), 0.5, 2.0),
        "spread_a": jnp.clip(jnp.exp(jax.random.uniform(key_of[2], (3, 2 * R + 1), jnp.float32, math.log(0.05), math.log(1.0))), 0.05, 1.0),
        "spread_b": jnp.clip(jnp.exp(jax.random.uniform(key_of[3], (3, 2 * R + 1), jnp.float32, math.log(0.05), math.log(1.0))), 0.05, 1.0),
    }


def band_table(weights, count_in, count_out, offset):
    source = jnp.arange(count_in, dtype=jnp.int32)[:, None]
    target = jnp.arange(count_out, dtype=jnp.int32)[None, :]
    spread = source - target + offset
    table = jnp.zeros((count_in, count_out), jnp.float32)
    for place in range(weights.shape[0]):
        table = table + jnp.where(spread == place, weights[place], jnp.float32(0.0))
    return table


def blur(volume, kernels):
    padded_x = jnp.pad(volume, ((0, 0), (0, 0), (R, R)))
    along_x = jnp.zeros_like(volume)
    for tap_index in range(2 * R + 1):
        along_x = along_x + kernels[2, tap_index] * padded_x[:, :, tap_index:tap_index + NX]
    table_y = band_table(kernels[1], NY, NY, R)
    along_y = jnp.einsum("zyx,yw->zwx", along_x, table_y, precision=lax.Precision.HIGHEST)
    padded = jnp.pad(along_y, ((R, R), (0, 0), (0, 0)))
    total = jnp.zeros_like(along_y)
    for tap_index in range(2 * R + 1):
        total = total + kernels[0, tap_index] * padded[tap_index:tap_index + NZ]
    return total


def reference(view_a, view_b_own, spread_a, spread_b):
    view_b = jnp.transpose(view_b_own, (2, 1, 0))[:, :, ::-1]
    blur_a = spread_a / jnp.sum(spread_a, axis=1, keepdims=True)
    blur_b = spread_b / jnp.sum(spread_b, axis=1, keepdims=True)
    estimate = 0.5 * (view_a + view_b)
    for iteration in range(ITERS):
        for measured, kernels in ((view_a, blur_a), (view_b, blur_b)):
            quotient = measured / blur(estimate, kernels)
            estimate = estimate * blur(quotient, kernels[:, ::-1])
    return estimate
```

```python
import functools

import jax
import jax.numpy as jnp
from jax import lax
from jax.experimental import pallas as pl
from jax.experimental.pallas import tpu as pltpu
from jax.sharding import PartitionSpec as P

LANES = 128
QUARTERS = 4


def padded(cells, sides, width):
    for axis, dim in sides:
        count = lax.axis_size(axis)
        ends = count - 1
        head = lax.slice_in_dim(cells, 0, width, axis=dim)
        tail = lax.slice_in_dim(cells, cells.shape[dim] - width, cells.shape[dim], axis=dim)
        cells = jnp.concatenate(
            [
                lax.ppermute(tail, axis, [(i, (i + 1) % count) for i in range(ends)]),
                cells,
                lax.ppermute(head, axis, [((i + 1) % count, i) for i in range(ends)]),
            ],
            axis=dim,
        )
    return cells


def band_table(weights, count_in, count_out, offset):
    source = jnp.arange(count_in, dtype=jnp.int32)[:, None]
    target = jnp.arange(count_out, dtype=jnp.int32)[None, :]
    spread = source - target + offset
    table = jnp.zeros((count_in, count_out), jnp.float32)
    for place in range(weights.shape[0]):
        table = table + jnp.where(spread == place, weights[place], jnp.float32(0.0))
    return table


def blur(volume, kernels):
    count_z, count_y, count_x = volume.shape
    radius = (kernels.shape[1] - 1) // 2
    table_x = band_table(kernels[2], count_x, count_x, radius)
    along_x = jnp.einsum("zyx,xw->zyw", volume, table_x, precision=lax.Precision.HIGHEST)
    table_y = band_table(kernels[1], count_y + 2 * radius, count_y, 0)
    widened = padded(along_x, (("gy", 1),), radius)
    narrow_y = jnp.einsum("zyx,yw->zwx", widened, table_y, precision=lax.Precision.HIGHEST)
    along_y = padded(narrow_y, (("gz", 0),), radius)
    table_z = band_table(kernels[0], count_z + 2 * radius, count_z, 0)
    return jnp.einsum("zyx,zw->wyx", along_y, table_z, precision=lax.Precision.HIGHEST)


def shards(view_a, view_b_own, spread_a, spread_b):
    arrived = lax.all_to_all(view_b_own, "gz", split_axis=2, concat_axis=0, tiled=True)
    view_b = jnp.transpose(arrived, (2, 1, 0))[:, :, ::-1]
    blur_a = spread_a / jnp.sum(spread_a, axis=1, keepdims=True)
    blur_b = spread_b / jnp.sum(spread_b, axis=1, keepdims=True)
    estimate = 0.5 * (view_a + view_b)
    for measured, kernels in ((view_a, blur_a), (view_b, blur_b)):
        quotient = measured / blur(estimate, kernels)
        estimate = estimate * blur(quotient, kernels[:, ::-1])
    return estimate


def block_transpose(parts, width):
    lane = lax.broadcasted_iota(jnp.int32, parts[0].shape, 1)
    for step in (2, 1):
        shift = step * width
        low = lax.rem(lane // shift, 2) == 0
        out = list(parts)
        for first in range(QUARTERS):
            if first & step:
                continue
            second = first + step
            out[first] = jnp.where(low, parts[first], pltpu.roll(parts[second], shift, 1))
            out[second] = jnp.where(low, pltpu.roll(parts[first], LANES - shift, 1), parts[second])
        parts = out
    return parts


def split(values):
    high = values.astype(jnp.bfloat16)
    return high, (values - high.astype(jnp.float32)).astype(jnp.bfloat16)


def dot(a, b):
    return jnp.dot(a, b, preferred_element_type=jnp.float32)


def deconvolve(
    va_ref, vb_ref, sa_ref, sb_ref, out_ref,
    send_a, recv_a, recv_b, view_a, view_b, estimate, blurred, work, halo_left, halo_right,
    send_e, recv_e, tz_high, tz_low, ty_high, ty_low,
    a_send_sem, a_recv_sem, b_sem, h_send_sem, h_recv_sem, e_send_sem, e_recv_sem,
):
    f32 = jnp.float32
    groups = lax.axis_size("gz")
    devices = 2 * groups
    block = lax.axis_index("blocks")
    gz, gy = lax.axis_index("gz"), lax.axis_index("gy")
    me = 2 * gz + gy
    slab = 2 * (groups - 1 - gz) + gy
    deep, tall, _ = va_ref.shape
    wide, full_y, full_z = view_a.shape
    taps = sa_ref.shape[1]
    radius = (taps - 1) // 2
    rows_y = tall // QUARTERS
    spreads = (sa_ref, sb_ref)

    def slab_of(device):
        return 2 * (groups - 1 - device // 2) + lax.rem(device, 2)

    def at(device):
        return (block, device // 2, lax.rem(device, 2))

    barrier = pltpu.get_barrier_semaphore()
    for hop in range(1, devices):
        pl.semaphore_signal(
            barrier, inc=1, device_id=at(lax.rem(me + hop, devices)), device_id_type=pl.DeviceIdType.MESH
        )

    for y in range(rows_y):
        for column in range(va_ref.shape[2] // LANES):
            parts = [
                va_ref[:, q * rows_y + y, column * LANES:(column + 1) * LANES] for q in range(QUARTERS)
            ]
            for k, part in enumerate(block_transpose(parts, wide)):
                send_a[QUARTERS * column + k, y] = part

    pl.semaphore_wait(barrier, devices - 1)

    half = pltpu.make_async_remote_copy(
        src_ref=vb_ref.at[pl.ds(wide * gy, wide)],
        dst_ref=recv_b,
        send_sem=b_sem.at[0],
        recv_sem=b_sem.at[1],
        device_id=(block, gz, 1 - gy),
        device_id_type=pl.DeviceIdType.MESH,
    )
    half.start()
    copies_a = []
    for hop in range(1, devices):
        target = lax.rem(me + hop, devices)
        copy = pltpu.make_async_remote_copy(
            src_ref=send_a.at[slab_of(target)],
            dst_ref=recv_a.at[gy, :, pl.ds(pl.multiple_of(gz * deep, 8), deep)],
            send_sem=a_send_sem.at[hop],
            recv_sem=a_recv_sem.at[hop],
            device_id=at(target),
            device_id_type=pl.DeviceIdType.MESH,
        )
        copy.start()
        copies_a.append(copy)
    recv_a[gy, :, pl.ds(pl.multiple_of(gz * deep, 8), deep)] = send_a[slab]

    row = lax.broadcasted_iota(jnp.int32, (full_z, LANES), 0)
    col = lax.broadcasted_iota(jnp.int32, (full_z, LANES), 1)
    for which, spread in enumerate(spreads):
        total = f32(1.0)
        for axis in range(3):
            line = spread[axis, 0]
            for tap in range(1, taps):
                line = line + spread[axis, tap]
            total = total * line
        for flipped in range(2):
            index = 2 * which + flipped
            sign = -1 if flipped else 1
            offset = sign * (row - col) + radius
            table = jnp.zeros((full_z, LANES), f32)
            for tap in range(taps):
                table = jnp.where(offset == tap, spread[0, tap], table)
            table = table / jnp.full((full_z, LANES), total, f32)
            tz_high[index], tz_low[index] = split(table)
            offset = jnp.where(row // full_y == col // full_y, sign * (col - row) + radius, -1)
            table = jnp.zeros((LANES, LANES), f32)
            for tap in range(taps):
                table = jnp.where(offset == tap, spread[1, tap], table)
            ty_high[index], ty_low[index] = split(table)

    mine, other = pl.multiple_of(gy * tall, 8), pl.multiple_of((1 - gy) * tall, 8)
    for x in range(wide):
        view_b[x, pl.ds(mine, tall)] = vb_ref[2 * wide - 1 - wide * gy - x]
    half.wait()
    for x in range(wide):
        view_b[x, pl.ds(other, tall)] = recv_b[wide - 1 - x]

    for copy in copies_a:
        copy.wait_recv()
    for side in range(2):
        for y in range(rows_y):
            turned = recv_a[side, y].T
            for q in range(QUARTERS):
                view_a[:, side * tall + q * rows_y + y, :] = turned[q * wide:(q + 1) * wide]

    planes = LANES // full_y
    chunks = wide // planes

    def along_zy(values, index):
        high, low = split(values.reshape(LANES, full_z))
        zh = tz_high[index]
        done = dot(high, zh) + (dot(low, zh) + dot(high, tz_low[index]))
        high, low = split(done)
        yh = ty_high[index]
        done = dot(yh, high) + (dot(yh, low) + dot(ty_low[index], high))
        return done.reshape(planes, full_y, full_z)

    has_left, has_right = slab > 0, slab < devices - 1

    def device_of(place):
        return (block, groups - 1 - place // 2, lax.rem(place, 2))

    left, right = device_of(jnp.maximum(slab - 1, 0)), device_of(jnp.minimum(slab + 1, devices - 1))

    def x_taps(turn, spread, flipped, source, first, outputs, fresh):
        count = source.shape[0]

        def body(part, carry):
            ys = pl.ds(pl.multiple_of(part * 8, 8), 8)
            weights = [spread[2, taps - 1 - tap if flipped else tap] for tap in range(taps)]
            for x in outputs:
                total = None if fresh else blurred[x, ys]
                for tap in range(taps):
                    place = x + tap - radius - first
                    if 0 <= place < count:
                        term = weights[tap] * source[place, ys]
                        total = term if total is None else total + term
                blurred[x, ys] = total
            return carry

        lax.fori_loop(0, full_y // 8, body, 0)

    def blur(turn, which, flipped, values):
        index = 2 * which + flipped
        spread = spreads[which]
        held = work.at[turn]
        to_left = pltpu.make_async_remote_copy(
            src_ref=held.at[pl.ds(0, radius)],
            dst_ref=halo_right.at[turn],
            send_sem=h_send_sem.at[turn, 0],
            recv_sem=h_recv_sem.at[turn, 0],
            device_id=left,
            device_id_type=pl.DeviceIdType.MESH,
        )
        to_right = pltpu.make_async_remote_copy(
            src_ref=held.at[pl.ds(wide - radius, radius)],
            dst_ref=halo_left.at[turn],
            send_sem=h_send_sem.at[turn, 1],
            recv_sem=h_recv_sem.at[turn, 1],
            device_id=right,
            device_id_type=pl.DeviceIdType.MESH,
        )
        for chunk in range(chunks):
            span = pl.ds(chunk * planes, planes)
            held[span] = along_zy(values(span), index)
            if chunk == (radius - 1) // planes:
                pl.when(has_left)(to_left.start)
        pl.when(has_right)(to_right.start)
        x_taps(turn, spread, flipped, held, 0, range(wide), True)

        @pl.when(has_left)
        def _():
            to_right.wait_recv()
            x_taps(turn, spread, flipped, halo_left.at[turn], -radius, range(radius), False)

        @pl.when(has_right)
        def _():
            to_left.wait_recv()
            x_taps(turn, spread, flipped, halo_right.at[turn], wide, range(wide - radius, wide), False)

        pl.when(has_left)(to_left.wait_send)
        pl.when(has_right)(to_right.wait_send)

    def start_values(span):
        estimate[span] = 0.5 * (view_a[span] + view_b[span])
        return estimate[span]

    def next_values(span):
        estimate[span] = estimate[span] * blurred[span]
        return estimate[span]

    blur(0, 0, 0, start_values)
    blur(1, 0, 1, lambda span: view_a[span] / blurred[span])
    blur(2, 1, 0, next_values)
    blur(3, 1, 1, lambda span: view_b[span] / blurred[span])
    for chunk in range(chunks):
        next_values(pl.ds(chunk * planes, planes))

    for side in range(2):
        for y in range(rows_y):
            lines = [estimate[:, side * tall + q * rows_y + y, :] for q in range(QUARTERS)]
            send_e[side, y] = jnp.concatenate(lines, axis=0).T
    copies_e = []
    for hop in range(1, devices):
        target = lax.rem(me + hop, devices)
        copy = pltpu.make_async_remote_copy(
            src_ref=send_e.at[lax.rem(target, 2), :, pl.ds(pl.multiple_of(target // 2 * deep, 8), deep)],
            dst_ref=recv_e.at[slab],
            send_sem=e_send_sem.at[hop],
            recv_sem=e_recv_sem.at[hop],
            device_id=at(target),
            device_id_type=pl.DeviceIdType.MESH,
        )
        copy.start()
        copies_e.append(copy)
    recv_e[slab] = send_e[gy, :, pl.ds(pl.multiple_of(gz * deep, 8), deep)]
    for copy in copies_e:
        copy.wait_recv()
    for y in range(rows_y):
        for column in range(va_ref.shape[2] // LANES):
            parts = [recv_e[QUARTERS * column + k, y] for k in range(QUARTERS)]
            for q, part in enumerate(block_transpose(parts, wide)):
                out_ref[q * rows_y + y, :, column * LANES:(column + 1) * LANES] = part
    for copy in copies_a + copies_e:
        copy.wait_send()


def slab_shards(view_a, view_b_own, spread_a, spread_b):
    groups = lax.axis_size("gz")
    deep, tall, long_x = view_a.shape
    devices = 2 * groups
    wide = long_x // devices
    full_y, full_z = 2 * tall, view_b_own.shape[2]
    taps = spread_a.shape[1]
    radius = (taps - 1) // 2
    f32, bf16 = jnp.float32, jnp.bfloat16
    volume = pltpu.VMEM((wide, full_y, full_z), f32)
    rows_y = tall // QUARTERS
    turned = pl.pallas_call(
        deconvolve,
        out_shape=jax.ShapeDtypeStruct((tall, deep, long_x), f32),
        in_specs=[pl.BlockSpec(memory_space=pltpu.VMEM)] * 2 + [pl.BlockSpec(memory_space=pltpu.SMEM)] * 2,
        out_specs=pl.BlockSpec(memory_space=pltpu.VMEM),
        scratch_shapes=[
            pltpu.VMEM((devices, rows_y, deep, LANES), f32),
            pltpu.VMEM((2, rows_y, full_z, LANES), f32),
            pltpu.VMEM((wide, tall, full_z), f32),
            volume, volume, volume, volume,
            pltpu.VMEM((4, wide, full_y, full_z), f32),
            pltpu.VMEM((4, radius, full_y, full_z), f32),
            pltpu.VMEM((4, radius, full_y, full_z), f32),
            pltpu.VMEM((2, rows_y, full_z, LANES), f32),
            pltpu.VMEM((devices, rows_y, deep, LANES), f32),
            pltpu.VMEM((4, full_z, full_z), bf16), pltpu.VMEM((4, full_z, full_z), bf16),
            pltpu.VMEM((4, LANES, LANES), bf16), pltpu.VMEM((4, LANES, LANES), bf16),
            pltpu.SemaphoreType.DMA((devices,)), pltpu.SemaphoreType.DMA((devices,)),
            pltpu.SemaphoreType.DMA((2,)),
            pltpu.SemaphoreType.DMA((4, 2)), pltpu.SemaphoreType.DMA((4, 2)),
            pltpu.SemaphoreType.DMA((devices,)), pltpu.SemaphoreType.DMA((devices,)),
        ],
        compiler_params=pltpu.CompilerParams(
            collective_id=0, has_side_effects=True, vmem_limit_bytes=48 * 1024 * 1024
        ),
    )(view_a, view_b_own, spread_a, spread_b)
    return jnp.transpose(turned, (1, 0, 2))


def fits_slabs(mesh, view_a, view_b_own, spread_a):
    groups, sides = mesh.shape["gz"], mesh.shape["gy"]
    deep = view_a[0] // (mesh.shape["blocks"] * groups)
    tall, wide = view_a[1] // sides, view_a[2] // (2 * groups)
    return (
        sides == 2 and wide * QUARTERS == LANES and view_b_own[2] == LANES and 4 * view_a[1] == LANES
        and tall % (8 * sides) == 0 and deep % 8 == 0 and spread_a[1] % 2 == 1 and spread_a[1] // 2 <= wide // 2
    )


def solution(mesh):
    in_specs = (P(("blocks", "gz"), "gy", None), P(("blocks", "gz"), "gy", None), P(), P())
    out_specs = P(("blocks", "gz"), "gy", None)

    def run(view_a, view_b_own, spread_a, spread_b):
        plan = slab_shards if fits_slabs(mesh, view_a.shape, view_b_own.shape, spread_a.shape) else shards
        split_plan = jax.shard_map(plan, mesh=mesh, in_specs=in_specs, out_specs=out_specs, check_vma=False)
        return split_plan(view_a, view_b_own, spread_a, spread_b)

    return run
```
